32 devices in a mesh: dp: 2 (over x), tp: 16 (over y, z, core).
Axes of the slice: x: 2, y: 2, z: 4, core: 2. Of those that a mesh axis runs over, the one named last changes fastest.
Arguments:
- x: bfloat16 [4096, 8192], P(('dp', 'tp')), parts along dimension 0
- w_gate: bfloat16 [8192, 32768], P(None, 'tp')
- w_up: bfloat16 [8192, 32768], P(None, 'tp')
- w_down: bfloat16 [32768, 8192], P('tp')
Outputs:
- output: bfloat16 [4096, 8192], P(('dp', 'tp')), parts along dimension 0
There are 2 independent parts. The reference program is written for one: setup_inputs(seed, part) draws one part's arguments, and reference() takes and returns one part's arrays. A program takes and returns all parts, laid end to end along the dimension named above; an argument that names none is the same for every part.
All inputs are finite; a program needn't handle non-finite values.
Results may differ from the reference program's by a relative error of at most 0.016.
Values are sent between devices in bfloat16 or wider.
A program may use at most 2 GiB of HBM per device.

```python
import jax
import jax.numpy as jnp

ROWS = 2048
D = 8192
FF = 32768


def setup_inputs(seed: int = 0, part: int = 0) -> dict:
    kx, kg, ku, kd = jax.random.split(jax.random.key(seed), 4)
    drawn = {
        "x": jax.random.normal(jax.random.fold_in(kx, part), (ROWS, D), jnp.float32),
        "w_gate": jax.random.normal(kg, (D, FF), jnp.float32) * D**-0.5,
        "w_up": jax.random.normal(ku, (D, FF), jnp.float32) * D**-0.5,
        "w_down": jax.random.normal(kd, (FF, D), jnp.float32) * FF**-0.5,
    }
    return {k: v.astype(jnp.bfloat16) for k, v in drawn.items()}


def reference(x, w_gate, w_up, w_down):
    gate = jnp.dot(x, w_gate, preferred_element_type=jnp.float32)
    up = jnp.dot(x, w_up, preferred_element_type=jnp.float32)
    hidden = (jax.nn.silu(gate) * up).astype(jnp.bfloat16)
    return jnp.dot(hidden, w_down, preferred_element_type=jnp.float32).astype(jnp.bfloat16)
```

```python
import functools

import jax
import jax.numpy as jnp
from jax import lax
from jax.experimental import pallas as pl
from jax.experimental.pallas import tpu as pltpu
from jax.sharding import PartitionSpec as P

MESH = pl.DeviceIdType.MESH
CHIPS = 8
TILES = 8
AGS_AT = 1
XL_AT = 6


def place():
    me = lax.axis_index("tp")
    core, chip = lax.rem(me, 2), lax.div(me, 2)
    y, z = lax.div(chip, 4), lax.rem(chip, 4)
    position = y * z + (1 - y) * (7 - z)

    def device(q):
        upper = lax.div(q, 4)
        return ((1 - upper) * (4 + q) + upper * (7 - q)) * 2 + core

    right = device(lax.rem(position + 1, CHIPS))
    left = device(lax.rem(position + CHIPS - 1, CHIPS))
    return core, right, left, chip * 2 + 1 - core


def kernel(
    x_ref, wg_ref, wu_ref, wd_ref, y_ref, xg_ref,
    xv, wgu, wdv, hid, acc, sib_out, sib_in, ring_out, ring_in, yv,
    x_sem, gu_sem, d_sem, ag_send, ag_recv, sx_send, sx_recv, so_send, so_recv, ro_send, ro_recv, y_sem,
):
    core, right, left, sib = place()
    mine = x_ref.shape[0]
    half = mine // 2
    tf, td = wgu.shape[3], wdv.shape[2]

    def remote(src, dst, send, recv, device):
        return pltpu.make_async_remote_copy(
            src_ref=src, dst_ref=dst, send_sem=send, recv_sem=recv, device_id={"tp": device}, device_id_type=MESH
        )

    def ag(src, k, way):
        rows = pl.ds(way * half, half)
        s = x_ref.at[rows] if src is None else xg_ref.at[src, core, rows]
        return remote(s, xg_ref.at[k + 1, core, rows], ag_send.at[k, way], ag_recv.at[k, way], (right, left)[way])

    def sx(src, k):
        s = x_ref if src is None else xg_ref.at[src, core]
        return remote(s, xg_ref.at[k, core], sx_send.at[k], sx_recv.at[k], sib)

    def load_mine(k):
        s = x_ref if k is None else xg_ref.at[k, core]
        return pltpu.make_async_copy(s, xv.at[pl.ds(0, mine)], x_sem.at[0])

    def load_other(k):
        return pltpu.make_async_copy(xg_ref.at[k, 1 - core], xv.at[pl.ds(mine, mine)], x_sem.at[1])

    def gu(j, slot):
        columns = pl.ds(pl.multiple_of(j * tf, tf), tf)
        return (
            pltpu.make_async_copy(wg_ref.at[:, columns], wgu.at[slot, 0], gu_sem.at[slot, 0]),
            pltpu.make_async_copy(wu_ref.at[:, columns], wgu.at[slot, 1], gu_sem.at[slot, 1]),
        )

    def start_gu(j, slot):
        for c in gu(j, slot):
            c.start()

    def down(n, slot):
        columns = pl.ds(pl.multiple_of(n * td, td), td)
        return pltpu.make_async_copy(wd_ref.at[:, columns], wdv.at[slot], d_sem.at[slot])

    def to_sib(parity, n):
        return remote(
            sib_out.at[lax.rem(n, 2)], sib_in.at[parity, n], so_send.at[lax.rem(n, 2)], so_recv.at[parity, n], sib
        )

    def to_ring(k, m, way):
        rows = pl.ds(way * half, half)
        return remote(
            ring_out.at[lax.rem(m, 2), rows],
            ring_in.at[k, m, rows],
            ro_send.at[lax.rem(m, 2), way],
            ro_recv.at[k, m, way],
            (right, left)[way],
        )

    def project(slot, more):
        def tile(j, _):
            now = lax.rem(j, 2)

            def ahead():
                start_gu(lax.rem(j + 1, TILES), 1 - now)

            if more:
                ahead()
            else:
                pl.when(j < TILES - 1)(ahead)
            for c in gu(j, now):
                c.wait()
            gate = jnp.dot(xv[...], wgu[now, 0], preferred_element_type=jnp.float32)
            up = jnp.dot(xv[...], wgu[now, 1], preferred_element_type=jnp.float32)
            columns = pl.ds(pl.multiple_of(j * tf, tf), tf)
            hid[slot, :, columns] = (jax.nn.silu(gate) * up).astype(jnp.bfloat16)
            return 0

        lax.fori_loop(0, TILES, tile, 0)

    def arrive(k):
        for way in range(2):
            ag(0, k - 1, way).wait_recv()

            @pl.when(k < CHIPS - 1)
            def _():
                ag(k, k, way).start()

        sx(k, k).start()

    def fetch(k):
        sx(k, k).wait_recv()
        load_mine(k).start()
        load_other(k).start()

    def sums(k, last):
        slot = 0 if last else 1
        parity = lax.rem(k, 2)

        def tile(n, _):
            now = lax.rem(n, 2)

            @pl.when(n < TILES)
            def _():
                if last:
                    pl.when(n < TILES - 1)(lambda: down(n + 1, 1 - now).start())
                else:
                    pl.when((n < TILES - 1) | (k == CHIPS - 1))(
                        lambda: down(lax.rem(n + 1, TILES), 1 - now).start()
                    )
                down(n, now).wait()
                term = jnp.dot(hid[slot], wdv[now], preferred_element_type=jnp.float32)
                acc[now] = term[:mine]
                if last:
                    to_sib(parity, n).wait_send()
                else:
                    pl.when((k > 1) | (n >= 2))(lambda: to_sib(parity, n).wait_send())
                sib_out[now] = term[mine:].astype(jnp.bfloat16)
                to_sib(parity, n).start()

            if not last:

                @pl.when((n == AGS_AT) & (k < CHIPS - 1))
                def _():
                    arrive(k + 1)

                @pl.when((n == XL_AT) & (k < CHIPS - 1))
                def _():
                    fetch(k + 1)

            @pl.when(n >= 1)
            def _():
                m = n - 1
                then = 1 - now
                to_sib(parity, m).wait_recv()
                if last:
                    for way in range(2):
                        to_ring(k - 1, m, way).wait_recv()
                    pl.when(m >= 2)(lambda: out(m).wait())
                    total = acc[then] + sib_in[parity, m].astype(jnp.float32)
                    total = total + ring_in[k - 1, m].astype(jnp.float32)
                    yv[then] = total.astype(jnp.bfloat16)
                    out(m).start()
                else:

                    @pl.when((k > 1) | (m >= 2))
                    def _():
                        for way in range(2):
                            to_ring(k, m, way).wait_send()

                    @pl.when(k == 1)
                    def _():
                        total = acc[then] + sib_in[parity, m].astype(jnp.float32)
                        ring_out[then] = total.astype(jnp.bfloat16)

                    @pl.when(k > 1)
                    def _():
                        for way in range(2):
                            to_ring(k - 1, m, way).wait_recv()
                        total = acc[then] + sib_in[parity, m].astype(jnp.float32)
                        total = total + ring_in[k - 1, m].astype(jnp.float32)
                        ring_out[then] = total.astype(jnp.bfloat16)

                    for way in range(2):
                        to_ring(k, m, way).start()

            return 0

        lax.fori_loop(0, TILES + 1, tile, 0)

    def out(m):
        columns = pl.ds(pl.multiple_of(m * td, td), td)
        return pltpu.make_async_copy(yv.at[lax.rem(m, 2)], y_ref.at[:, columns], y_sem.at[lax.rem(m, 2)])

    start_gu(0, 0)
    load_mine(None).start()
    barrier = pltpu.get_barrier_semaphore()
    for partner in (left, right, sib):
        pl.semaphore_signal(barrier, inc=1, device_id={"tp": partner}, device_id_type=MESH)
    pl.semaphore_wait(barrier, 3)

    sx(None, 0).start()
    for way in range(2):
        ag(None, 0, way).start()
    sx(None, 0).wait_recv()
    load_other(0).start()
    load_mine(None).wait()
    load_other(0).wait()
    project(0, True)
    arrive(1)
    fetch(1)

    def step(k, _):
        down(0, 0).start()
        load_mine(k).wait()
        load_other(k).wait()
        project(1, False)
        pl.when(k < CHIPS - 1)(lambda: start_gu(0, 0))
        sums(k, False)
        return 0

    lax.fori_loop(1, CHIPS, step, 0)
    sums(CHIPS, True)

    for n in range(2):
        to_sib(0, n).wait_send()
        for way in range(2):
            to_ring(CHIPS - 1, n, way).wait_send()
        out(n).wait()

    def sent(k, _):
        sx(k, k).wait_send()
        return 0

    lax.fori_loop(0, CHIPS, sent, 0)

    def sent_on(k, _):
        for way in range(2):
            ag(k, k, way).wait_send()
        return 0

    lax.fori_loop(0, CHIPS - 1, sent_on, 0)


def block(x, w_gate, w_up, w_down):
    mine, d = x.shape
    f = w_gate.shape[1]
    tf, td = f // TILES, d // TILES
    bf16, dma = jnp.bfloat16, pltpu.SemaphoreType.DMA
    hbm = pl.BlockSpec(memory_space=pl.ANY)
    y, _ = pl.pallas_call(
        kernel,
        out_shape=(
            jax.ShapeDtypeStruct((mine, d), bf16),
            jax.ShapeDtypeStruct((CHIPS, 2, mine, d), bf16),
        ),
        in_specs=[hbm] * 4,
        out_specs=(hbm, hbm),
        scratch_shapes=[
            pltpu.VMEM((2 * mine, d), bf16),
            pltpu.VMEM((2, 2, d, tf), bf16),
            pltpu.VMEM((2, f, td), bf16),
            pltpu.VMEM((2, 2 * mine, f), bf16),
            pltpu.VMEM((2, mine, td), jnp.float32),
            pltpu.VMEM((2, mine, td), bf16),
            pltpu.VMEM((2, TILES, mine, td), bf16),
            pltpu.VMEM((2, mine, td), bf16),
            pltpu.VMEM((CHIPS, TILES, mine, td), bf16),
            pltpu.VMEM((2, mine, td), bf16),
            dma((2,)),
            dma((2, 2)),
            dma((2,)),
            dma((CHIPS - 1, 2)),
            dma((CHIPS - 1, 2)),
            dma((CHIPS,)),
            dma((CHIPS,)),
            dma((2,)),
            dma((2, TILES)),
            dma((2, 2)),
            dma((CHIPS, TILES, 2)),
            dma((2,)),
        ],
        compiler_params=pltpu.CompilerParams(
            collective_id=0, has_side_effects=True, vmem_limit_bytes=67_043_328
        ),
        cost_estimate=pl.CostEstimate(
            flops=6 * CHIPS * 2 * mine * d * f,
            bytes_accessed=CHIPS * 6 * d * f,
            transcendentals=CHIPS * 2 * mine * f,
        ),
    )(x, w_gate, w_up, w_down)
    return y


def solution(mesh):
    return jax.shard_map(
        block,
        mesh=mesh,
        in_specs=(P(("dp", "tp"), None), P(None, "tp"), P(None, "tp"), P("tp", None)),
        out_specs=P(("dp", "tp"), None),
        check_vma=False,
    )
```

```python
import functools

import jax
import jax.numpy as jnp
from jax import lax
from jax.experimental import pallas as pl
from jax.experimental.pallas import tpu as pltpu
from jax.sharding import PartitionSpec as P

MESH = pl.DeviceIdType.MESH
CHIPS = 8
TILES = 8
PIECES = 4
SLOTS = 7
LAG = 2
XL_AT = 2
FIRST = 2 * TILES
STEP = 3 * TILES
LAST = FIRST + (CHIPS - 1) * STEP


def place():
    me = lax.axis_index("tp")
    core, chip = lax.rem(me, 2), lax.div(me, 2)
    y, z = lax.div(chip, 4), lax.rem(chip, 4)
    position = y * z + (1 - y) * (7 - z)

    def device(q):
        upper = lax.div(q, 4)
        return ((1 - upper) * (4 + q) + upper * (7 - q)) * 2 + core

    right = device(lax.rem(position + 1, CHIPS))
    left = device(lax.rem(position + CHIPS - 1, CHIPS))
    return core, right, left, chip * 2 + 1 - core


def kernel(
    x_ref, wg_ref, wu_ref, wd_ref, y_ref, xg_ref,
    xv, w, hid, acc, sib_out, sib_in, ring_out, ring_in, yv,
    x_sem, w_sem, ag_send, ag_recv, sx_send, sx_recv, so_send, so_recv, ro_send, ro_recv, y_sem,
):
    core, right, left, sib = place()
    mine = x_ref.shape[0]
    half = mine // 2
    piece = half // PIECES
    f, tf = hid.shape[2], w.shape[2]
    td = acc.shape[2]
    parts = td // tf

    def remote(src, dst, send, recv, device):
        return pltpu.make_async_remote_copy(
            src_ref=src, dst_ref=dst, send_sem=send, recv_sem=recv, device_id={"tp": device}, device_id_type=MESH
        )

    def rows_of(way, p):
        return pl.ds(pl.multiple_of(way * half + p * piece, piece), piece)

    def ag(src, k, p, way):
        rows = rows_of(way, p)
        s = x_ref.at[rows] if src is None else xg_ref.at[src, core, rows]
        return remote(s, xg_ref.at[k + 1, core, rows], ag_send.at[k], ag_recv.at[k, p, way], (right, left)[way])

    def sx(src, k, rows):
        s = x_ref.at[rows] if src is None else xg_ref.at[src, core, rows]
        return remote(s, xg_ref.at[k, core, rows], sx_send.at[k], sx_recv.at[k], sib)

    everything = pl.ds(0, mine)

    def load_mine(k):
        s = x_ref if k is None else xg_ref.at[k, core]
        return pltpu.make_async_copy(s, xv.at[pl.ds(0, mine)], x_sem.at[0])

    def load_other(k):
        return pltpu.make_async_copy(xg_ref.at[k, 1 - core], xv.at[pl.ds(mine, mine)], x_sem.at[1])

    def start_weights(i):
        slot = lax.rem(i, SLOTS)
        r = i - FIRST
        q = jnp.where(i < FIRST, i, jnp.where(i < LAST, lax.rem(r, STEP), i - LAST + FIRST))

        def columns(j):
            return pl.ds(pl.multiple_of(j * tf, tf), tf)

        @pl.when((q < FIRST) & (lax.rem(q, 2) == 0))
        def _():
            pltpu.make_async_copy(wg_ref.at[:, columns(lax.div(q, 2))], w.at[slot], w_sem.at[slot]).start()

        @pl.when((q < FIRST) & (lax.rem(q, 2) == 1))
        def _():
            pltpu.make_async_copy(wu_ref.at[:, columns(lax.div(q, 2))], w.at[slot], w_sem.at[slot]).start()

        @pl.when((q >= FIRST) & (i < LAST + TILES))
        def _():
            for part in range(parts):
                pltpu.make_async_copy(
                    wd_ref.at[:, columns((q - FIRST) * parts + part)],
                    w.at[slot, pl.ds(part * f, f)],
                    w_sem.at[slot],
                ).start()

    def wait_weights(i):
        slot = lax.rem(i, SLOTS)
        pltpu.make_async_copy(wg_ref.at[:, pl.ds(0, tf)], w.at[slot], w_sem.at[slot]).wait()
        return slot

    def to_sib(parity, n):
        t = lax.rem(n, LAG + 1)
        return remote(sib_out.at[t], sib_in.at[parity, n], so_send.at[t], so_recv.at[parity, n], sib)

    def to_ring(k, m, way):
        rows = pl.ds(way * half, half)
        return remote(
            ring_out.at[m, rows], ring_in.at[k, m, rows], ro_send.at[m, way], ro_recv.at[k, m, way], (right, left)[way]
        )

    def arrive(k, p):
        for way in range(2):
            ag(0, k - 1, p, way).wait_recv()

            @pl.when(k < CHIPS - 1)
            def _():
                ag(k, k, p, way).start()

            sx(k, k, rows_of(way, p)).start()

    def fetch(k):
        sx(k, k, everything).wait_recv()
        load_mine(k).start()
        load_other(k).start()

    def project(slot, item, k):
        def tile(j, _):
            i = item + 2 * j
            start_weights(i + SLOTS - 2)
            start_weights(i + SLOTS - 1)
            g = wait_weights(i)
            u = wait_weights(i + 1)
            gate = jnp.dot(xv[...], w[g], preferred_element_type=jnp.float32)
            up = jnp.dot(xv[...], w[u], preferred_element_type=jnp.float32)
            columns = pl.ds(pl.multiple_of(j * tf, tf), tf)
            hid[slot, :, columns] = (jax.nn.silu(gate) * up).astype(jnp.bfloat16)

            @pl.when((lax.rem(j, TILES // PIECES) == TILES // PIECES - 1) & (k < CHIPS))
            def _():
                arrive(k, lax.div(j, TILES // PIECES))

            return 0

        lax.fori_loop(0, TILES, tile, 0)

    def sums(k, item, last):
        slot = 0 if last else 1
        parity = lax.rem(k, 2)

        def tile(n, _):
            @pl.when(n < TILES)
            def _():
                now = lax.rem(n, LAG + 1)
                i = item + n
                start_weights(i + SLOTS - 2)
                v = wait_weights(i)
                if last:
                    to_sib(parity, n).wait_send()
                else:
                    pl.when((k > 1) | (n >= LAG + 1))(lambda: to_sib(parity, n).wait_send())
                for part in range(parts):
                    term = jnp.dot(hid[slot], w[v, part * f : (part + 1) * f], preferred_element_type=jnp.float32)
                    acc[now, :, part * tf : (part + 1) * tf] = term[:mine]
                    sib_out[now, :, part * tf : (part + 1) * tf] = term[mine:].astype(jnp.bfloat16)
                to_sib(parity, n).start()

            if not last:

                @pl.when((n == XL_AT) & (k < CHIPS - 1))
                def _():
                    fetch(k + 1)

            @pl.when(n >= LAG)
            def _():
                m = n - LAG
                then = lax.rem(m, LAG + 1)
                t = lax.rem(m, 2)
                to_sib(parity, m).wait_recv()
                if last:
                    for way in range(2):
                        to_ring(k - 1, m, way).wait_recv()
                    pl.when(m >= 2)(lambda: out(m).wait())
                    total = acc[then] + sib_in[parity, m].astype(jnp.float32)
                    total = total + ring_in[k - 1, m].astype(jnp.float32)
                    yv[t] = total.astype(jnp.bfloat16)
                    out(m).start()
                else:

                    @pl.when(k > 1)
                    def _():
                        for way in range(2):
                            to_ring(k, m, way).wait_send()

                    @pl.when(k == 1)
                    def _():
                        total = acc[then] + sib_in[parity, m].astype(jnp.float32)
                        ring_out[m] = total.astype(jnp.bfloat16)

                    @pl.when(k > 1)
                    def _():
                        for way in range(2):
                            to_ring(k - 1, m, way).wait_recv()
                        total = acc[then] + sib_in[parity, m].astype(jnp.float32)
                        total = total + ring_in[k - 1, m].astype(jnp.float32)
                        ring_out[m] = total.astype(jnp.bfloat16)

                    for way in range(2):
                        to_ring(k, m, way).start()

            return 0

        lax.fori_loop(0, TILES + LAG, tile, 0)

    def out(m):
        columns = pl.ds(pl.multiple_of(m * td, td), td)
        return pltpu.make_async_copy(yv.at[lax.rem(m, 2)], y_ref.at[:, columns], y_sem.at[lax.rem(m, 2)])

    load_mine(None).start()
    for i in range(SLOTS - 2):
        start_weights(jnp.int32(i))
    barrier = pltpu.get_barrier_semaphore()
    for partner in (left, right, sib):
        pl.semaphore_signal(barrier, inc=1, device_id={"tp": partner}, device_id_type=MESH)
    pl.semaphore_wait(barrier, 3)

    sx(None, 0, everything).start()
    for p in range(PIECES):
        for way in range(2):
            ag(None, 0, p, way).start()
    sx(None, 0, everything).wait_recv()
    load_other(0).start()
    load_mine(None).wait()
    load_other(0).wait()
    project(0, 0, 1)
    fetch(1)

    def step(k, _):
        item = FIRST + (k - 1) * STEP
        load_mine(k).wait()
        load_other(k).wait()
        project(1, item, k + 1)
        sums(k, item + FIRST, False)
        return 0

    lax.fori_loop(1, CHIPS, step, 0)
    sums(CHIPS, LAST, True)

    for n in range(LAG + 1):
        to_sib(0, n).wait_send()
    for n in range(2):
        out(n).wait()

    def summed(m, _):
        for way in range(2):
            to_ring(CHIPS - 1, m, way).wait_send()
        return 0

    lax.fori_loop(0, TILES, summed, 0)

    def sent(k, _):
        sx(k, k, everything).wait_send()
        return 0

    lax.fori_loop(0, CHIPS, sent, 0)

    def sent_on(k, _):
        remote(x_ref, xg_ref.at[k, core], ag_send.at[k], sx_recv.at[k], sib).wait_send()
        return 0

    lax.fori_loop(0, CHIPS - 1, sent_on, 0)


def block(x, w_gate, w_up, w_down):
    mine, d = x.shape
    f = w_gate.shape[1]
    tf, td = f // TILES, d // TILES
    bf16, dma = jnp.bfloat16, pltpu.SemaphoreType.DMA
    hbm = pl.BlockSpec(memory_space=pl.ANY)
    y, _ = pl.pallas_call(
        kernel,
        out_shape=(
            jax.ShapeDtypeStruct((mine, d), bf16),
            jax.ShapeDtypeStruct((CHIPS, 2, mine, d), bf16),
        ),
        in_specs=[hbm] * 4,
        out_specs=(hbm, hbm),
        scratch_shapes=[
            pltpu.VMEM((2 * mine, d), bf16),
            pltpu.VMEM((SLOTS, d, tf), bf16),
            pltpu.VMEM((2, 2 * mine, f), bf16),
            pltpu.VMEM((LAG + 1, mine, td), jnp.float32),
            pltpu.VMEM((LAG + 1, mine, td), bf16),
            pltpu.VMEM((2, TILES, mine, td), bf16),
            pltpu.VMEM((TILES, mine, td), bf16),
            pltpu.VMEM((CHIPS, TILES, mine, td), bf16),
            pltpu.VMEM((2, mine, td), bf16),
            dma((2,)),
            dma((SLOTS,)),
            dma((CHIPS - 1,)),
            dma((CHIPS - 1, PIECES, 2)),
            dma((CHIPS,)),
            dma((CHIPS,)),
            dma((LAG + 1,)),
            dma((2, TILES)),
            dma((TILES, 2)),
            dma((CHIPS, TILES, 2)),
            dma((2,)),
        ],
        compiler_params=pltpu.CompilerParams(
            collective_id=0, has_side_effects=True, vmem_limit_bytes=67_043_328
        ),
        cost_estimate=pl.CostEstimate(
            flops=6 * CHIPS * 2 * mine * d * f,
            bytes_accessed=CHIPS * 6 * d * f,
            transcendentals=CHIPS * 2 * mine * f,
        ),
    )(x, w_gate, w_up, w_down)
    return y


def solution(mesh):
    return jax.shard_map(
        block,
        mesh=mesh,
        in_specs=(P(("dp", "tp"), None), P(None, "tp"), P(None, "tp"), P("tp", None)),
        out_specs=P(("dp", "tp"), None),
        check_vma=False,
    )
```

```python
import functools

import jax
import jax.numpy as jnp
from jax import lax
from jax.experimental import pallas as pl
from jax.experimental.pallas import tpu as pltpu
from jax.sharding import PartitionSpec as P

MESH = pl.DeviceIdType.MESH
CHIPS = 8
TILES = 8
PIECES = 4
SLOTS = 6
LAG = 2
XL_AT = 2
FIRST = 2 * TILES
STEP = 3 * TILES
LAST = FIRST + (CHIPS - 1) * STEP


def place():
    me = lax.axis_index("tp")
    core, chip = lax.rem(me, 2), lax.div(me, 2)
    y, z = lax.div(chip, 4), lax.rem(chip, 4)
    position = y * z + (1 - y) * (7 - z)

    def device(q):
        upper = lax.div(q, 4)
        return ((1 - upper) * (4 + q) + upper * (7 - q)) * 2 + core

    right = device(lax.rem(position + 1, CHIPS))
    left = device(lax.rem(position + CHIPS - 1, CHIPS))
    return core, right, left, chip * 2 + 1 - core


def kernel(
    x_ref, wg_ref, wu_ref, wd_ref, y_ref, xg_ref,
    xv, w, hid, acc, sib_out, sib_in, ring_out, ring_in, yv,
    x_sem, w_sem, ag_send, ag_recv, sx_send, sx_recv, so_send, so_recv, ro_send, ro_recv, y_sem,
):
    core, right, left, sib = place()
    mine = x_ref.shape[0]
    half = mine // 2
    piece = half // PIECES
    f, tf = hid.shape[2], w.shape[2]
    td = acc.shape[2]
    parts = td // tf

    def remote(src, dst, send, recv, device):
        return pltpu.make_async_remote_copy(
            src_ref=src, dst_ref=dst, send_sem=send, recv_sem=recv, device_id={"tp": device}, device_id_type=MESH
        )

    def rows_of(way, p):
        return pl.ds(pl.multiple_of(way * half + p * piece, piece), piece)

    def ag(src, k, p, way):
        rows = rows_of(way, p)
        s = x_ref.at[rows] if src is None else xg_ref.at[src, core, rows]
        return remote(s, xg_ref.at[k + 1, core, rows], ag_send.at[k], ag_recv.at[k, p, way], (right, left)[way])

    def sx(src, k, rows):
        s = x_ref.at[rows] if src is None else xg_ref.at[src, core, rows]
        return remote(s, xg_ref.at[k, core, rows], sx_send.at[k], sx_recv.at[k], sib)

    everything = pl.ds(0, mine)

    def load_mine(k):
        s = x_ref if k is None else xg_ref.at[k, core]
        return pltpu.make_async_copy(s, xv.at[pl.ds(0, mine)], x_sem.at[0])

    def load_other(k):
        return pltpu.make_async_copy(xg_ref.at[k, 1 - core], xv.at[pl.ds(mine, mine)], x_sem.at[1])

    def start_weights(i):
        slot = lax.rem(i, SLOTS)
        r = i - FIRST
        q = jnp.where(i < FIRST, i, jnp.where(i < LAST, lax.rem(r, STEP), i - LAST + FIRST))

        def columns(j):
            return pl.ds(pl.multiple_of(j * tf, tf), tf)

        @pl.when((q < FIRST) & (lax.rem(q, 2) == 0))
        def _():
            pltpu.make_async_copy(wg_ref.at[:, columns(lax.div(q, 2))], w.at[slot], w_sem.at[slot]).start()

        @pl.when((q < FIRST) & (lax.rem(q, 2) == 1))
        def _():
            pltpu.make_async_copy(wu_ref.at[:, columns(lax.div(q, 2))], w.at[slot], w_sem.at[slot]).start()

        @pl.when((q >= FIRST) & (i < LAST + TILES))
        def _():
            for part in range(parts):
                pltpu.make_async_copy(
                    wd_ref.at[:, columns((q - FIRST) * parts + part)],
                    w.at[slot, pl.ds(part * f, f)],
                    w_sem.at[slot],
                ).start()

    def wait_weights(i):
        slot = lax.rem(i, SLOTS)
        pltpu.make_async_copy(wg_ref.at[:, pl.ds(0, tf)], w.at[slot], w_sem.at[slot]).wait()
        return slot

    def to_sib(parity, n):
        return remote(sib_out.at[n], sib_in.at[parity, n], so_send.at[n], so_recv.at[parity, n], sib)

    def to_ring(k, m, way):
        rows = pl.ds(way * half, half)
        return remote(
            ring_out.at[m, rows],
            ring_in.at[k - 1, m, rows],
            ro_send.at[m, way],
            ro_recv.at[k - 1, m, way],
            (right, left)[way],
        )

    def arrive(k, p):
        for way in range(2):
            ag(0, k - 1, p, way).wait_recv()

            @pl.when(k < CHIPS - 1)
            def _():
                ag(k, k, p, way).start()

            sx(k, k, rows_of(way, p)).start()

    def fetch(k):
        sx(k, k, everything).wait_recv()
        load_mine(k).start()
        load_other(k).start()

    def combine(k, m):
        to_sib(lax.rem(k, 2), m).wait_recv()

        @pl.when(k == 1)
        def _():
            ring_out[m] = (acc[m] + sib_in[lax.rem(k, 2), m].astype(jnp.float32)).astype(jnp.bfloat16)

        @pl.when(k > 1)
        def _():
            for way in range(2):
                to_ring(k - 1, m, way).wait_send()
                to_ring(k - 1, m, way).wait_recv()
            total = acc[m] + sib_in[lax.rem(k, 2), m].astype(jnp.float32)
            ring_out[m] = (total + ring_in[k - 2, m].astype(jnp.float32)).astype(jnp.bfloat16)

        for way in range(2):
            to_ring(k, m, way).start()

    def finish(m):
        to_sib(0, m).wait_recv()
        for way in range(2):
            to_ring(CHIPS - 1, m, way).wait_recv()
        t = lax.rem(m, 2)
        pl.when(m >= 2)(lambda: out(m).wait())
        total = acc[m] + sib_in[0, m].astype(jnp.float32)
        yv[t] = (total + ring_in[CHIPS - 2, m].astype(jnp.float32)).astype(jnp.bfloat16)
        out(m).start()

    def project(slot, item, k):
        def tile(j, _):
            i = item + 2 * j
            start_weights(i + SLOTS - 2)
            start_weights(i + SLOTS - 1)
            g = wait_weights(i)
            u = wait_weights(i + 1)
            gate = jnp.dot(xv[...], w[g], preferred_element_type=jnp.float32)
            up = jnp.dot(xv[...], w[u], preferred_element_type=jnp.float32)
            columns = pl.ds(pl.multiple_of(j * tf, tf), tf)
            hid[slot, :, columns] = (jax.nn.silu(gate) * up).astype(jnp.bfloat16)

            @pl.when((lax.rem(j, TILES // PIECES) == TILES // PIECES - 1) & (k < CHIPS - 1))
            def _():
                arrive(k + 1, lax.div(j, TILES // PIECES))

            if slot:
                pl.when(k > 1)(lambda: combine(k - 1, j))
            return 0

        lax.fori_loop(0, TILES, tile, 0)

    def sums(k, item, last):
        slot = 0 if last else 1
        parity = lax.rem(k, 2)

        def tile(n, _):
            @pl.when(n < TILES)
            def _():
                i = item + n
                start_weights(i + SLOTS - 2)
                v = wait_weights(i)
                if last:
                    to_sib(parity, n).wait_send()
                else:
                    pl.when(k > 1)(lambda: to_sib(parity, n).wait_send())
                for part in range(parts):
                    term = jnp.dot(hid[slot], w[v, part * f : (part + 1) * f], preferred_element_type=jnp.float32)
                    acc[n, :, part * tf : (part + 1) * tf] = term[:mine]
                    sib_out[n, :, part * tf : (part + 1) * tf] = term[mine:].astype(jnp.bfloat16)
                to_sib(parity, n).start()

            if last:
                pl.when(n >= LAG)(lambda: finish(n - LAG))
            else:
                pl.when((n == XL_AT) & (k < CHIPS - 1))(lambda: fetch(k + 1))
                pl.when((n >= LAG) & (k == CHIPS - 1))(lambda: combine(k, n - LAG))
            return 0

        lax.fori_loop(0, TILES + LAG, tile, 0)

    def out(m):
        columns = pl.ds(pl.multiple_of(m * td, td), td)
        return pltpu.make_async_copy(yv.at[lax.rem(m, 2)], y_ref.at[:, columns], y_sem.at[lax.rem(m, 2)])

    load_mine(None).start()
    for i in range(SLOTS - 2):
        start_weights(jnp.int32(i))
    barrier = pltpu.get_barrier_semaphore()
    for partner in (left, right, sib):
        pl.semaphore_signal(barrier, inc=1, device_id={"tp": partner}, device_id_type=MESH)
    pl.semaphore_wait(barrier, 3)

    sx(None, 0, everything).start()
    for p in range(PIECES):
        for way in range(2):
            ag(None, 0, p, way).start()
    sx(None, 0, everything).wait_recv()
    load_other(0).start()
    load_mine(None).wait()
    load_other(0).wait()
    project(0, 0, 0)
    fetch(1)

    def step(k, _):
        item = FIRST + (k - 1) * STEP
        load_mine(k).wait()
        load_other(k).wait()
        project(1, item, k)
        sums(k, item + FIRST, False)
        return 0

    lax.fori_loop(1, CHIPS, step, 0)
    sums(CHIPS, LAST, True)

    for n in range(2):
        out(n).wait()

    def summed(m, _):
        to_sib(0, m).wait_send()
        for way in range(2):
            to_ring(CHIPS - 1, m, way).wait_send()
        return 0

    lax.fori_loop(0, TILES, summed, 0)

    def sent(k, _):
        sx(k, k, everything).wait_send()
        return 0

    lax.fori_loop(0, CHIPS, sent, 0)

    def sent_on(k, _):
        remote(x_ref, xg_ref.at[k, core], ag_send.at[k], sx_recv.at[k], sib).wait_send()
        return 0

    lax.fori_loop(0, CHIPS - 1, sent_on, 0)


def block(x, w_gate, w_up, w_down):
    mine, d = x.shape
    f = w_gate.shape[1]
    tf, td = f // TILES, d // TILES
    bf16, dma = jnp.bfloat16, pltpu.SemaphoreType.DMA
    hbm = pl.BlockSpec(memory_space=pl.ANY)
    y, _ = pl.pallas_call(
        kernel,
        out_shape=(
            jax.ShapeDtypeStruct((mine, d), bf16),
            jax.ShapeDtypeStruct((CHIPS, 2, mine, d), bf16),
        ),
        in_specs=[hbm] * 4,
        out_specs=(hbm, hbm),
        scratch_shapes=[
            pltpu.VMEM((2 * mine, d), bf16),
            pltpu.VMEM((SLOTS, d, tf), bf16),
            pltpu.VMEM((2, 2 * mine, f), bf16),
            pltpu.VMEM((TILES, mine, td), jnp.float32),
            pltpu.VMEM((TILES, mine, td), bf16),
            pltpu.VMEM((2, TILES, mine, td), bf16),
            pltpu.VMEM((TILES, mine, td), bf16),
            pltpu.VMEM((CHIPS - 1, TILES, mine, td), bf16),
            pltpu.VMEM((2, mine, td), bf16),
            dma((2,)),
            dma((SLOTS,)),
            dma((CHIPS - 1,)),
            dma((CHIPS - 1, PIECES, 2)),
            dma((CHIPS,)),
            dma((CHIPS,)),
            dma((TILES,)),
            dma((2, TILES)),
            dma((TILES, 2)),
            dma((CHIPS - 1, TILES, 2)),
            dma((2,)),
        ],
        compiler_params=pltpu.CompilerParams(
            collective_id=0, has_side_effects=True, vmem_limit_bytes=67_043_328
        ),
        cost_estimate=pl.CostEstimate(
            flops=6 * CHIPS * 2 * mine * d * f,
            bytes_accessed=CHIPS * 6 * d * f,
            transcendentals=CHIPS * 2 * mine * f,
        ),
    )(x, w_gate, w_up, w_down)
    return y


def solution(mesh):
    return jax.shard_map(
        block,
        mesh=mesh,
        in_specs=(P(("dp", "tp"), None), P(None, "tp"), P(None, "tp"), P("tp", None)),
        out_specs=P(("dp", "tp"), None),
        check_vma=False,
    )
```
